32 devices in a mesh: tp: 8 (over z, y), rep: 4 (over x, core).
Axes of the slice: x: 2, y: 2, z: 4, core: 2. Of those that a mesh axis runs over, the one named last changes fastest.
Arguments:
- tokens: bfloat16 [1536, 8192], P('rep', 'tp'), may hold values from -6 to 6
- row_lengths: int32 [8], P('rep'), may hold values from 1 to 192
- attn_gain: float32 [8192], P('tp'), may hold values from 0.1 to 1.9
- query_weight: bfloat16 [8192, 4096], P('rep', 'tp'), may hold values from -2 to 2
- key_weight: bfloat16 [8192, 512], P('rep', 'tp'), may hold values from -2 to 2
- value_matrix: bfloat16 [8192, 512], P('rep', 'tp'), may hold values from -0.0625 to 0.0625
- output_weight: bfloat16 [4096, 8192], P('rep', 'tp'), may hold values from -0.09375 to 0.09375
- final_gain: float32 [8192], P('tp'), may hold values from 0.1 to 1.9
- value_head: float32 [8192, 6], P('tp'), may hold values from -0.0625 to 0.0625
Outputs:
- resid_out: bfloat16 [1536, 8192], P('rep', 'tp')
- objective_scores: float32 [1536, 6], P('rep')
The draws below stay inside these ranges and needn't reach their ends.
All inputs are finite; a program needn't handle non-finite values.
Results may differ from the reference program's by a relative error of at most 0.025.
Values may be sent and summed in bfloat16 or wider, within the bound.
A program may use at most 64 MiB of HBM per device.

```python
import math
import jax
import jax.numpy as jnp
from jax import lax

MODEL_WIDTH = 8192
QUERY_HEADS = 32
KEY_VALUE_HEADS = 4
HEAD_SIZE = 128
NOBJ = 6
ROW_LENGTH = 192
TOKENS = 1536
SEQS = 8


def shared_keys(key):
    return jax.random.normal(jax.random.fold_in(key, 11), (MODEL_WIDTH, KEY_VALUE_HEADS * HEAD_SIZE), jnp.float32) / math.sqrt(MODEL_WIDTH)


def draw_key_weight(key, part):
    return jnp.clip(shared_keys(key), -2.0, 2.0).astype(jnp.bfloat16)


def draw_query_weight(key, part):
    noise = jax.random.normal(jax.random.fold_in(key, 23), (MODEL_WIDTH, QUERY_HEADS * HEAD_SIZE), jnp.float32) / math.sqrt(MODEL_WIDTH)
    return jnp.clip(noise, -2.0, 2.0).astype(jnp.bfloat16)


def set_ends(array, stream_key, least, high):
    longest = array.shape.index(max(array.shape))
    spots = []
    for shift in (0, 1):
        where = [jax.random.randint(jax.random.fold_in(stream_key, axis), (), 0, length) for axis, length in enumerate(array.shape)]
        where[longest] = (where[longest] + shift) % array.shape[longest]
        spots.append(tuple(where))
    return array.at[spots[0]].set(least).at[spots[1]].set(high)


def shard_levels(stream_key, dims, cuts, smallest, high):
    def one(dim, shards_of):
        draws = jax.random.uniform(jax.random.fold_in(jax.random.fold_in(stream_key, 6), dim), (shards_of,), jnp.float32, smallest / len(cuts), high / len(cuts))
        return jnp.repeat(jnp.exp(draws), dims[dim] // shards_of).reshape((-1,) + (1,) * (len(dims) - dim - 1))

    factor_of = one(*cuts[0])
    for cut in cuts[1:]:
        factor_of = factor_of * one(*cut)
    return factor_of


def normal_values(rng, dims, width, reach, split=(), held_as=jnp.bfloat16):
    level = shard_levels(rng, dims, split, -0.22, 0.18) if split else 1.0
    values = jax.random.normal(rng, dims, jnp.float32) * width * level
    return jnp.minimum(jnp.maximum(values, -reach), reach).astype(held_as)


def setup_inputs(seed: int = 0) -> dict:
    key_list = jax.random.split(jax.random.key(seed), 10)
    return {
        "tokens": normal_values(key_list[0], (TOKENS, MODEL_WIDTH), 1.0, 6.0, ((0, 4), (1, 8))),
        "row_lengths": set_ends(jax.random.randint(key_list[1], (SEQS,), 1, ROW_LENGTH + 1), jax.random.fold_in(key_list[1], 1), 1, ROW_LENGTH).astype(jnp.int32),
        "attn_gain": jnp.clip(1.0 + 0.18 * jax.random.normal(key_list[2], (MODEL_WIDTH,), jnp.float32), 0.1, 1.9),
        "query_weight": draw_query_weight(jax.random.fold_in(key_list[9], 71), 0),
        "key_weight": draw_key_weight(jax.random.fold_in(key_list[9], 71), 0),
        "value_matrix": normal_values(key_list[5], (MODEL_WIDTH, KEY_VALUE_HEADS * HEAD_SIZE), MODEL_WIDTH ** -0.5, 0.0625, ((0, 4), (1, 8))),
        "output_weight": normal_values(key_list[6], (QUERY_HEADS * HEAD_SIZE, MODEL_WIDTH), (QUERY_HEADS * HEAD_SIZE) ** -0.5, 0.09375, ((0, 4), (1, 8))),
        "final_gain": jnp.clip(1.0 + 0.18 * jax.random.normal(key_list[7], (MODEL_WIDTH,), jnp.float32), 0.1, 1.9),
        "value_head": normal_values(key_list[8], (MODEL_WIDTH, NOBJ), MODEL_WIDTH ** -0.5, 0.0625, ((0, 8),), jnp.float32),
    }


EPS = 1e-05

def reference(tokens, row_lengths, attn_gain, query_weight, key_weight, value_matrix, output_weight, final_gain, value_head):
    xf = tokens.astype(jnp.float32)
    first_scale = lax.rsqrt(lax.optimization_barrier(jnp.mean(xf * xf, axis=1, keepdims=True)) + EPS)
    normed = (xf * first_scale * attn_gain).astype(jnp.bfloat16)
    query = jnp.dot(normed, query_weight, preferred_element_type=jnp.float32).astype(jnp.bfloat16)
    key_rows = jnp.dot(normed, key_weight, preferred_element_type=jnp.float32).astype(jnp.bfloat16)
    value_rows = jnp.dot(normed, value_matrix, preferred_element_type=jnp.float32).astype(jnp.bfloat16)
    every_row = tokens.shape[0] // ROW_LENGTH
    query4 = query.reshape(every_row, ROW_LENGTH, QUERY_HEADS, HEAD_SIZE)
    key_tensor4 = key_rows.reshape(every_row, ROW_LENGTH, KEY_VALUE_HEADS, HEAD_SIZE)
    value_tensor4 = value_rows.reshape(every_row, ROW_LENGTH, KEY_VALUE_HEADS, HEAD_SIZE)
    position = jnp.arange(ROW_LENGTH, dtype=jnp.int32)
    causal = position[None, :] <= position[:, None]
    allowed = causal[None, :, :] & (position[None, None, :] < row_lengths[:, None, None])
    inv_root = 1.0 / HEAD_SIZE ** 0.5

    def one_head(index):
        qpart = lax.dynamic_index_in_dim(query4, index, 2, keepdims=False).astype(jnp.float32)
        shared = (index % KEY_VALUE_HEADS).astype(jnp.int32)
        kpart = lax.dynamic_index_in_dim(key_tensor4, shared, 2, keepdims=False).astype(jnp.float32)
        vpart = lax.dynamic_index_in_dim(value_tensor4, shared, 2, keepdims=False).astype(jnp.float32)
        scores = jnp.einsum('rqd,rkd->rqk', qpart, kpart) * inv_root
        scores = jnp.where(allowed, scores, jnp.float32(-1e+30))
        scores = scores - lax.optimization_barrier(jnp.max(scores, axis=2, keepdims=True))
        expo = jnp.exp(scores)
        probs = (expo / lax.optimization_barrier(jnp.sum(expo, axis=2, keepdims=True))).astype(jnp.bfloat16)
        probs = lax.optimization_barrier(probs).astype(jnp.float32)
        return jnp.einsum('rqk,rkd->rqd', probs, vpart).astype(jnp.bfloat16)
    heads = lax.map(one_head, jnp.arange(QUERY_HEADS, dtype=jnp.int32))
    attended = jnp.transpose(heads, (1, 2, 0, 3)).reshape(tokens.shape[0], QUERY_HEADS * HEAD_SIZE)
    update = jnp.dot(attended, output_weight, preferred_element_type=jnp.float32)
    resid_out = (xf + update).astype(jnp.bfloat16)
    rfloat = resid_out.astype(jnp.float32)
    final_scale = lax.rsqrt(lax.optimization_barrier(jnp.mean(rfloat * rfloat, axis=1, keepdims=True)) + EPS)
    weighted = jnp.dot(rfloat * final_gain, value_head, precision=lax.Precision.HIGHEST)
    logits = weighted * final_scale
    live = (position[None, :] < row_lengths[:, None]).reshape(tokens.shape[0], 1)
    objective_scores = jnp.where(live, logits, jnp.float32(0.0))
    return (resid_out, objective_scores)
```

```python
import functools
import jax
import jax.numpy as jnp
from jax import lax
from jax.experimental import pallas as pl
from jax.experimental.pallas import tpu as pltpu
from jax.sharding import PartitionSpec as P

KEY_VALUE_HEADS = 4
HEAD_SIZE = 128
EPS = 1e-05
MESH = pl.DeviceIdType.MESH


def slot(ref, dim, size, index):
    if dim is None:
        return ref.at[index]
    start = pl.multiple_of(index * size, size)
    return ref.at[pl.ds(start, size)] if dim == 0 else ref.at[:, pl.ds(start, size)]


class Line:
    def __init__(self, axis, count, dim, src, dst, sems):
        self.axis, self.dim, self.src, self.dst = axis, dim, src, dst
        self.count = count
        self.up_sem, self.down_sem, self.pair_sem, self.line_recv, self.pair_recv, self.own_sem = sems
        me = lax.axis_index(axis)
        self.me, self.place, self.side = me, me // 2, me % 2
        self.partner = me + 1 - 2 * self.side
        self.size = None if dim is None else src.shape[dim]

    def at(self, index):
        return slot(self.dst, self.dim, self.size, index)

    def copy(self, source, index, send, recv, target):
        return pltpu.make_async_remote_copy(
            src_ref=source,
            dst_ref=self.at(index),
            send_sem=send,
            recv_sem=recv,
            device_id={self.axis: target},
            device_id_type=MESH,
        )

    def up(self, source, origin):
        return self.copy(
            source, 2 * origin + self.side, self.up_sem.at[origin], self.line_recv.at[origin], self.me + 2
        )

    def down(self, source, origin):
        return self.copy(
            source, 2 * origin + self.side, self.down_sem.at[origin], self.line_recv.at[origin], self.me - 2
        )

    def pair(self, source, origin):
        return self.copy(
            source,
            2 * origin + self.side,
            self.pair_sem.at[origin],
            self.pair_recv.at[origin],
            self.partner,
        )

    def own(self):
        return pltpu.make_async_copy(self.src, self.at(self.me), self.own_sem.at[0])

    def has_up(self):
        return self.place < self.count - 1

    def has_down(self):
        return self.place > 0

    def begin(self):
        @pl.when(self.has_up())
        def _():
            self.up(self.src, self.place).start()

        @pl.when(self.has_down())
        def _():
            self.down(self.src, self.place).start()

        self.pair(self.src, self.place).start()
        self.own().start()

    def hop(self, step):
        below, above = self.place - step, self.place + step

        @pl.when(below >= 0)
        def _():
            block = self.at(2 * below + self.side)
            self.up(block, below).wait_recv()

            @pl.when(self.has_up())
            def _():
                self.up(block, below).start()

            self.pair(block, below).start()

        @pl.when(above < self.count)
        def _():
            block = self.at(2 * above + self.side)
            self.down(block, above).wait_recv()

            @pl.when(self.has_down())
            def _():
                self.down(block, above).start()

            self.pair(block, above).start()

    def finish(self):
        self.own().wait()
        for origin in range(self.count):
            here = self.at(2 * origin + self.side)
            self.pair(here, origin).wait_send()
            pltpu.make_async_remote_copy(
                src_ref=here,
                dst_ref=self.at(2 * origin + 1 - self.side),
                send_sem=self.pair_sem.at[origin],
                recv_sem=self.pair_recv.at[origin],
                device_id={self.axis: self.partner},
                device_id_type=MESH,
            ).wait_recv()

            @pl.when((origin <= self.place) & self.has_up())
            def _():
                self.up(here, origin).wait_send()

            @pl.when((origin >= self.place) & self.has_down())
            def _():
                self.down(here, origin).wait_send()

    def neighbours(self):
        return ((self.has_up(), self.me + 2), (self.has_down(), self.me - 2), (None, self.partner))


class Direct:
    def __init__(self, axis, members, src, dst, sems):
        self.axis, self.members, self.src, self.dst = axis, members, src, dst
        self.send, self.recv, self.own_sem = sems
        self.me = lax.axis_index(axis)

    def to(self, offset):
        return pltpu.make_async_remote_copy(
            src_ref=self.src,
            dst_ref=self.dst.at[self.me],
            send_sem=self.send.at[offset - 1],
            recv_sem=self.recv.at[offset - 1],
            device_id={self.axis: lax.rem(self.me + offset, self.members)},
            device_id_type=MESH,
        )

    def come(self, offset):
        return pltpu.make_async_remote_copy(
            src_ref=self.src,
            dst_ref=self.dst.at[lax.rem(self.me - offset + self.members, self.members)],
            send_sem=self.send.at[offset - 1],
            recv_sem=self.recv.at[offset - 1],
            device_id={self.axis: lax.rem(self.me + offset, self.members)},
            device_id_type=MESH,
        )

    def own(self):
        return pltpu.make_async_copy(self.src, self.dst.at[self.me], self.own_sem.at[0])

    def begin(self):
        for offset in range(1, self.members):
            self.to(offset).start()
        self.own().start()

    def finish(self):
        for offset in range(1, self.members):
            self.to(offset).wait_send()
            self.come(offset).wait_recv()
        self.own().wait()


def gather_kernel(plan, sizes, *refs):
    count = len(plan)
    sources, targets = refs[:count], refs[count : 2 * count]
    sems = list(refs[2 * count :])
    jobs = []
    for (kind, axis, dim), src, dst in zip(plan, sources, targets):
        if kind == "line":
            jobs.append(Line(axis, sizes[axis] // 2, dim, src, dst, sems[:6]))
            del sems[:6]
        else:
            jobs.append(Direct(axis, sizes[axis], src, dst, sems[:3]))
            del sems[:3]
    barrier = pltpu.get_barrier_semaphore()
    direct_axes = {job.axis for job in jobs if isinstance(job, Direct)}
    greeted, peers = set(), 0
    for job in jobs:
        if job.axis in greeted:
            continue
        greeted.add(job.axis)
        if job.axis in direct_axes:
            members = sizes[job.axis]
            peers = peers + members - 1
            for offset in range(1, members):
                pl.semaphore_signal(
                    barrier,
                    inc=1,
                    device_id={job.axis: lax.rem(job.me + offset, members)},
                    device_id_type=MESH,
                )
        else:
            for there, target in job.neighbours():
                def signal(target=target, job=job):
                    pl.semaphore_signal(
                        barrier, inc=1, device_id={job.axis: target}, device_id_type=MESH
                    )

                if there is None:
                    peers = peers + 1
                    signal()
                else:
                    peers = peers + there.astype(jnp.int32)
                    pl.when(there)(signal)
    pl.semaphore_wait(barrier, peers)
    for job in jobs:
        job.begin()
    lines = [job for job in jobs if isinstance(job, Line)]
    for step in range(1, max([job.count for job in lines], default=1)):
        for job in lines:
            if step < job.count:
                job.hop(step)
    for job in jobs:
        job.finish()


def gather(plan, sizes, arrays, collective_id, memory=pl.ANY):
    shapes, scratch = [], []
    for (kind, axis, dim), array in zip(plan, arrays):
        members = sizes[axis]
        if dim is None:
            shape = (members,) + array.shape
        else:
            shape = tuple(n * members if i == dim else n for i, n in enumerate(array.shape))
        shapes.append(jax.ShapeDtypeStruct(shape, array.dtype))
        if kind == "line":
            scratch += [pltpu.SemaphoreType.DMA((members // 2,))] * 5
        else:
            scratch += [pltpu.SemaphoreType.DMA((members - 1,))] * 2
        scratch += [pltpu.SemaphoreType.DMA((1,))]
    return pl.pallas_call(
        functools.partial(gather_kernel, plan, sizes),
        out_shape=tuple(shapes),
        in_specs=[pl.BlockSpec(memory_space=memory)] * len(arrays),
        out_specs=tuple([pl.BlockSpec(memory_space=memory)] * len(arrays)),
        scratch_shapes=scratch,
        compiler_params=pltpu.CompilerParams(collective_id=collective_id, has_side_effects=True),
    )(*arrays)


def local(
    sizes,
    tokens,
    row_lengths,
    attn_gain,
    query_weight,
    key_weight,
    value_matrix,
    output_weight,
    final_gain,
    value_head,
):
    width = tokens.shape[1] * sizes["tp"]
    rows_here = tokens.shape[0]
    head_cols = query_weight.shape[1]
    kv_cols = key_weight.shape[1]
    xfloat = tokens.astype(jnp.float32)
    squares_here = jnp.sum(xfloat * xfloat, axis=1)[None, :]
    gained = (xfloat * attn_gain).astype(jnp.bfloat16)
    packed = jnp.concatenate([query_weight, key_weight, value_matrix], axis=1)
    columns, weights, squares_all = gather(
        (("line", "tp", 1), ("line", "rep", 0), ("direct", "tp", None)),
        sizes,
        (gained, packed, squares_here),
        0,
    )
    first_scale = lax.rsqrt(jnp.sum(squares_all, axis=(0, 1)) / width + EPS)[:, None]
    projected = jnp.dot(columns, weights, preferred_element_type=jnp.float32)
    projected = (projected * first_scale).astype(jnp.bfloat16)
    query = projected[:, :head_cols]
    (kv_all,) = gather((("line", "tp", None),), sizes, (projected[:, head_cols:],), 1)
    sequence_rows = row_lengths.shape[0]
    length = rows_here // sequence_rows
    local_heads = head_cols // HEAD_SIZE
    key_full = kv_all[:, :, :kv_cols].transpose(1, 0, 2).reshape(rows_here, -1)
    value_full = kv_all[:, :, kv_cols:].transpose(1, 0, 2).reshape(rows_here, -1)
    first_head = lax.axis_index("tp") * local_heads
    key_value_index = (first_head + jnp.arange(local_heads, dtype=jnp.int32)) % KEY_VALUE_HEADS
    query4 = query.reshape(sequence_rows, length, local_heads, HEAD_SIZE)
    key4 = key_full.reshape(sequence_rows, length, KEY_VALUE_HEADS, HEAD_SIZE)
    value4 = value_full.reshape(sequence_rows, length, KEY_VALUE_HEADS, HEAD_SIZE)
    if local_heads % KEY_VALUE_HEADS or local_heads != KEY_VALUE_HEADS:
        key4 = jnp.take(key4, key_value_index, axis=2)
        value4 = jnp.take(value4, key_value_index, axis=2)
    scores = jnp.einsum(
        "rqhd,rkhd->rhqk", query4, key4, preferred_element_type=jnp.float32
    ) * (1.0 / HEAD_SIZE**0.5)
    position = jnp.arange(length, dtype=jnp.int32)
    causal = position[None, :] <= position[:, None]
    allowed = causal[None, None, :, :] & (
        position[None, None, None, :] < row_lengths[:, None, None, None]
    )
    scores = jnp.where(allowed, scores, jnp.float32(-1e30))
    scores = scores - jnp.max(scores, axis=3, keepdims=True)
    expo = jnp.exp(scores)
    probs = (expo / jnp.sum(expo, axis=3, keepdims=True)).astype(jnp.bfloat16)
    attended = jnp.einsum(
        "rhqk,rkhd->rqhd", probs, value4, preferred_element_type=jnp.float32
    )
    attended = attended.astype(jnp.bfloat16).reshape(rows_here, head_cols)
    mixed, out_weights = gather(
        (("line", "tp", 1), ("line", "rep", 0)), sizes, (attended, output_weight), 2
    )
    update = jnp.dot(mixed, out_weights, preferred_element_type=jnp.float32)
    resid_out = (xfloat + update).astype(jnp.bfloat16)
    rfloat = resid_out.astype(jnp.float32)
    squares = jnp.sum(rfloat * rfloat, axis=1)
    local_scores = jnp.dot(rfloat * final_gain, value_head, precision=lax.Precision.HIGHEST)
    stats = jnp.concatenate([local_scores.T, squares[None, :]], axis=0)
    (stats_all,) = gather((("direct", "tp", None),), sizes, (stats,), 3)
    stats = jnp.sum(stats_all, axis=0)
    logits = (stats[:-1] * lax.rsqrt(stats[-1:] / width + EPS)).T
    live = (position[None, :] < row_lengths[:, None]).reshape(rows_here, 1)
    objective_scores = jnp.where(live, logits, jnp.float32(0.0))
    return (resid_out, objective_scores)


def solution(mesh):
    in_specs = (
        P("rep", "tp"),
        P("rep"),
        P("tp"),
        P("rep", "tp"),
        P("rep", "tp"),
        P("rep", "tp"),
        P("rep", "tp"),
        P("tp"),
        P("tp", None),
    )
    out_specs = (P("rep", "tp"), P("rep", None))
    body = functools.partial(local, dict(mesh.shape))
    return jax.shard_map(body, mesh=mesh, in_specs=in_specs, out_specs=out_specs, check_vma=False)
```

```python
import functools
import jax
import jax.numpy as jnp
from jax import lax
from jax.experimental import pallas as pl
from jax.experimental.pallas import tpu as pltpu
from jax.sharding import PartitionSpec as P

KEY_VALUE_HEADS = 4
HEAD_SIZE = 128
EPS = 1e-05
MESH = pl.DeviceIdType.MESH


class Stage:
    def __init__(self, src, dst, buffer, sems):
        self.into = pltpu.make_async_copy(src, buffer, sems.at[0])
        self.out = pltpu.make_async_copy(buffer, dst, sems.at[1])


def slot(ref, dim, size, index, rows=None):
    if rows is not None:
        return ref.at[pl.ds(*rows), pl.ds(pl.multiple_of(index * size, size), size)]
    if dim is None:
        return ref.at[index]
    if isinstance(dim, tuple):
        return ref.at[index, pl.ds(dim[2], dim[1])]
    start = pl.multiple_of(index * size, size)
    return ref.at[pl.ds(start, size)] if dim == 0 else ref.at[:, pl.ds(start, size)]


class Line:
    def __init__(self, axis, count, dim, src, dst, sems, rows=None):
        self.axis, self.dim, self.dst = axis, dim, dst
        self.windowed = isinstance(dim, tuple)
        rows = dim[:2] if self.windowed else rows
        self.src = src if rows is None else src.at[pl.ds(*rows)]
        self.rows = None if self.windowed else rows
        self.count = count
        self.up_sem, self.down_sem, self.pair_sem, self.line_recv, self.pair_recv = sems
        me = lax.axis_index(axis)
        self.me, self.place, self.side = me, me // 2, me % 2
        self.partner = me + 1 - 2 * self.side
        self.size = None if dim is None or self.windowed else src.shape[dim]

    def at(self, index):
        return slot(self.dst, self.dim, self.size, index, self.rows)

    def copy(self, source, index, send, recv, target):
        return pltpu.make_async_remote_copy(
            src_ref=source,
            dst_ref=self.at(index),
            send_sem=send,
            recv_sem=recv,
            device_id={self.axis: target},
            device_id_type=MESH,
        )

    def up(self, source, origin):
        return self.copy(
            source, 2 * origin + self.side, self.up_sem.at[origin], self.line_recv.at[origin], self.me + 2
        )

    def down(self, source, origin):
        return self.copy(
            source, 2 * origin + self.side, self.down_sem.at[origin], self.line_recv.at[origin], self.me - 2
        )

    def pair(self, source, origin):
        return self.copy(
            source,
            2 * origin + self.side,
            self.pair_sem.at[origin],
            self.pair_recv.at[origin],
            self.partner,
        )

    def own_block(self):
        return self.at(self.me)

    def has_up(self):
        return self.place < self.count - 1

    def has_down(self):
        return self.place > 0

    def begin(self):
        @pl.when(self.has_up())
        def _():
            self.up(self.src, self.place).start()

        @pl.when(self.has_down())
        def _():
            self.down(self.src, self.place).start()

        self.pair(self.src, self.place).start()

    def hop(self, step):
        below, above = self.place - step, self.place + step

        @pl.when(below >= 0)
        def _():
            block = self.at(2 * below + self.side)
            self.up(block, below).wait_recv()

            @pl.when(self.has_up())
            def _():
                self.up(block, below).start()

            self.pair(block, below).start()

        @pl.when(above < self.count)
        def _():
            block = self.at(2 * above + self.side)
            self.down(block, above).wait_recv()

            @pl.when(self.has_down())
            def _():
                self.down(block, above).start()

            self.pair(block, above).start()

    def finish(self):
        for origin in range(self.count):
            here = self.at(2 * origin + self.side)
            self.pair(here, origin).wait_send()
            pltpu.make_async_remote_copy(
                src_ref=here,
                dst_ref=self.at(2 * origin + 1 - self.side),
                send_sem=self.pair_sem.at[origin],
                recv_sem=self.pair_recv.at[origin],
                device_id={self.axis: self.partner},
                device_id_type=MESH,
            ).wait_recv()

            @pl.when((origin <= self.place) & self.has_up())
            def _():
                self.up(here, origin).wait_send()

            @pl.when((origin >= self.place) & self.has_down())
            def _():
                self.down(here, origin).wait_send()

    def neighbours(self):
        return ((self.has_up(), self.me + 2), (self.has_down(), self.me - 2), (None, self.partner))


class Cross(Line):
    def __init__(self, axis, count, dim, src, dst, sems, rows):
        super().__init__(axis, count, dim, src, dst, sems, rows)
        self.other = 1 - self.side

    def along(self, source, origin, side, which, step):
        sem = self.up_sem if step > 0 else self.down_sem
        return self.copy(
            source,
            2 * origin + side,
            sem.at[which * self.count + origin],
            self.line_recv.at[which * self.count + origin],
            self.me + step,
        )

    def spread(self, source, origin, which):
        side = self.side if which == 0 else self.other

        @pl.when(self.has_up() & (origin <= self.place))
        def _():
            self.along(source, origin, side, which, 2).start()

        @pl.when(self.has_down() & (origin >= self.place))
        def _():
            self.along(source, origin, side, which, -2).start()

    def across(self, index, source):
        return self.copy(source, index, self.pair_sem.at[0], self.pair_recv.at[0], self.partner)

    def begin(self):
        self.across(self.me, self.src).start()
        self.spread(self.src, self.place, 0)

    def turn(self):
        theirs = self.at(self.partner)
        self.across(self.partner, theirs).wait_recv()
        self.spread(theirs, self.place, 1)

    def hop(self, step):
        for which in range(2):
            side = self.side if which == 0 else self.other
            for origin in (self.place - step, self.place + step):

                @pl.when((origin >= 0) & (origin < self.count))
                def _(origin=origin, side=side, which=which):
                    block = self.at(2 * origin + side)
                    self.along(block, origin, side, which, 2).wait_recv()
                    self.spread(block, origin, which)

    def finish(self):
        self.across(self.me, self.src).wait_send()
        for which in range(2):
            side = self.side if which == 0 else self.other
            for origin in range(self.count):
                block = self.at(2 * origin + side)

                @pl.when((origin <= self.place) & self.has_up())
                def _(origin=origin, side=side, which=which, block=block):
                    self.along(block, origin, side, which, 2).wait_send()

                @pl.when((origin >= self.place) & self.has_down())
                def _(origin=origin, side=side, which=which, block=block):
                    self.along(block, origin, side, which, -2).wait_send()


class Direct:
    def __init__(self, axis, members, src, dst, sems):
        self.axis, self.members, self.src, self.dst = axis, members, src, dst
        self.send, self.recv = sems
        self.me = lax.axis_index(axis)

    def to(self, offset):
        return pltpu.make_async_remote_copy(
            src_ref=self.src,
            dst_ref=self.dst.at[self.me],
            send_sem=self.send.at[offset - 1],
            recv_sem=self.recv.at[offset - 1],
            device_id={self.axis: lax.rem(self.me + offset, self.members)},
            device_id_type=MESH,
        )

    def come(self, offset):
        return pltpu.make_async_remote_copy(
            src_ref=self.src,
            dst_ref=self.dst.at[lax.rem(self.me - offset + self.members, self.members)],
            send_sem=self.send.at[offset - 1],
            recv_sem=self.recv.at[offset - 1],
            device_id={self.axis: lax.rem(self.me + offset, self.members)},
            device_id_type=MESH,
        )

    def own_block(self):
        return self.dst.at[self.me]

    def begin(self):
        for offset in range(1, self.members):
            self.to(offset).start()

    def finish(self):
        for offset in range(1, self.members):
            self.to(offset).wait_send()
            self.come(offset).wait_recv()


def gather_kernel(plan, sizes, *refs):
    count = len(plan)
    sources, targets = refs[:count], refs[count : 2 * count]
    rest = list(refs[2 * count :])

    def take(number):
        taken = rest[:number]
        del rest[:number]
        return taken

    jobs, stages = [], []
    for (kind, axis, dim), src, dst in zip(plan, sources, targets):
        if kind == "fill":
            dst = targets[dim]
            buffer, sems = take(2)
            stages.append(Stage(src, dst.at[:, pl.ds(0, src.shape[1])], buffer, sems))
            continue
        if kind == "direct":
            made = [Direct(axis, sizes[axis], src, dst, take(2))]
        elif kind == "line":
            made = [Line(axis, sizes[axis] // 2, dim, src, dst, take(5))]
        else:
            first, second = cut(src.shape[0])
            made = [
                Line(axis, sizes[axis] // 2, dim, src, dst, take(5), first),
                Cross(axis, sizes[axis] // 2, dim, src, dst, take(5), second),
            ]
        for job in made:
            buffer, sems = take(2)
            stages.append(Stage(job.src, job.own_block(), buffer, sems))
        jobs += made
    barrier = pltpu.get_barrier_semaphore()
    direct_axes = {job.axis for job in jobs if isinstance(job, Direct)}
    greeted, peers = set(), 0
    for job in jobs:
        if job.axis in greeted:
            continue
        greeted.add(job.axis)
        if job.axis in direct_axes:
            members = sizes[job.axis]
            peers = peers + members - 1
            for offset in range(1, members):
                pl.semaphore_signal(
                    barrier,
                    inc=1,
                    device_id={job.axis: lax.rem(job.me + offset, members)},
                    device_id_type=MESH,
                )
        else:
            for there, target in job.neighbours():
                def signal(target=target, job=job):
                    pl.semaphore_signal(
                        barrier, inc=1, device_id={job.axis: target}, device_id_type=MESH
                    )

                if there is None:
                    peers = peers + 1
                    signal()
                else:
                    peers = peers + there.astype(jnp.int32)
                    pl.when(there)(signal)
    pl.semaphore_wait(barrier, peers)
    for job in jobs:
        job.begin()
    for stage in stages:
        stage.into.start()
    for stage in stages:
        stage.into.wait()
        stage.out.start()
    for job in jobs:
        if isinstance(job, Cross):
            job.turn()
    for axis in ("tp", "rep"):
        lines = [job for job in jobs if isinstance(job, Line) and job.axis == axis]
        for step in range(1, max([job.count for job in lines], default=1)):
            for job in lines:
                job.hop(step)
    for job in jobs:
        job.finish()
    for stage in stages:
        stage.out.wait()


def cut(total):
    cross = total // (6 * 16) * 16
    return (0, total - cross), (total - cross, cross)


def gather(plan, sizes, arrays, collective_id, memory=pl.ANY):
    shapes, scratch = [], []
    dma = pltpu.SemaphoreType.DMA
    for (kind, axis, dim), array in zip(plan, arrays):
        if kind == "fill":
            shapes.append(jax.ShapeDtypeStruct((8, 128), array.dtype))
            scratch += [pltpu.VMEM(array.shape, array.dtype), dma((2,))]
            continue
        members = sizes[axis]
        if dim is None:
            shape = (members,) + array.shape
        elif isinstance(dim, tuple):
            shape = (members, dim[2] + dim[1]) + array.shape[1:]
        else:
            shape = tuple(n * members if i == dim else n for i, n in enumerate(array.shape))
        shapes.append(jax.ShapeDtypeStruct(shape, array.dtype))
        whole = pltpu.VMEM(array.shape, array.dtype)
        if kind == "direct":
            scratch += [dma((members - 1,))] * 2 + [whole, dma((2,))]
        elif kind == "line":
            if isinstance(dim, tuple):
                whole = pltpu.VMEM(dim[1:2] + array.shape[1:], array.dtype)
            scratch += [dma((members // 2,))] * 5 + [whole, dma((2,))]
        else:
            scratch += [dma((members // 2,))] * 5 + [dma((members,))] * 5
            for _, length in cut(array.shape[0]):
                scratch += [pltpu.VMEM((length,) + array.shape[1:], array.dtype), dma((2,))]
    return pl.pallas_call(
        functools.partial(gather_kernel, plan, sizes),
        out_shape=tuple(shapes),
        in_specs=[pl.BlockSpec(memory_space=memory)] * len(arrays),
        out_specs=tuple([pl.BlockSpec(memory_space=memory)] * len(arrays)),
        scratch_shapes=scratch,
        compiler_params=pltpu.CompilerParams(collective_id=collective_id, has_side_effects=True),
    )(*arrays)


def local(
    sizes,
    tokens,
    row_lengths,
    attn_gain,
    query_weight,
    key_weight,
    value_matrix,
    output_weight,
    final_gain,
    value_head,
):
    width = tokens.shape[1] * sizes["tp"]
    rows_here = tokens.shape[0]
    head_cols = query_weight.shape[1]
    kv_cols = key_weight.shape[1]
    xfloat = tokens.astype(jnp.float32)
    squares_here = jnp.sum(xfloat * xfloat, axis=1)[None, :]
    gained = (xfloat * attn_gain).astype(jnp.bfloat16)
    packed = jnp.concatenate([query_weight, key_weight, value_matrix], axis=1)
    early = output_weight.shape[0] // 4
    columns, weights, squares_all = gather(
        (
            ("split", "tp", 1),
            ("line", "rep", 0),
            ("direct", "tp", None),
        ),
        sizes,
        (gained, packed, squares_here),
        0,
    )
    first_scale = lax.rsqrt(jnp.sum(squares_all, axis=(0, 1)) / width + EPS)[:, None]
    projected = jnp.dot(columns, weights, preferred_element_type=jnp.float32)
    projected = (projected * first_scale).astype(jnp.bfloat16)
    query = projected[:, :head_cols]
    kv_all, out_early = gather(
        (("line", "tp", None), ("line", "rep", (0, early, 0))),
        sizes,
        (projected[:, head_cols:], output_weight),
        1,
    )
    sequence_rows = row_lengths.shape[0]
    length = rows_here // sequence_rows
    local_heads = head_cols // HEAD_SIZE
    key_full = kv_all[:, :, :kv_cols].transpose(1, 0, 2).reshape(rows_here, -1)
    value_full = kv_all[:, :, kv_cols:].transpose(1, 0, 2).reshape(rows_here, -1)
    first_head = lax.axis_index("tp") * local_heads
    key_value_index = (first_head + jnp.arange(local_heads, dtype=jnp.int32)) % KEY_VALUE_HEADS
    query4 = query.reshape(sequence_rows, length, local_heads, HEAD_SIZE)
    key4 = key_full.reshape(sequence_rows, length, KEY_VALUE_HEADS, HEAD_SIZE)
    value4 = value_full.reshape(sequence_rows, length, KEY_VALUE_HEADS, HEAD_SIZE)
    if local_heads % KEY_VALUE_HEADS or local_heads != KEY_VALUE_HEADS:
        key4 = jnp.take(key4, key_value_index, axis=2)
        value4 = jnp.take(value4, key_value_index, axis=2)
    scores = jnp.einsum(
        "rqhd,rkhd->rhqk", query4, key4, preferred_element_type=jnp.float32
    ) * (1.0 / HEAD_SIZE**0.5)
    position = jnp.arange(length, dtype=jnp.int32)
    causal = position[None, :] <= position[:, None]
    allowed = causal[None, None, :, :] & (
        position[None, None, None, :] < row_lengths[:, None, None, None]
    )
    scores = jnp.where(allowed, scores, jnp.float32(-1e30))
    scores = scores - jnp.max(scores, axis=3, keepdims=True)
    expo = jnp.exp(scores)
    probs = (expo / jnp.sum(expo, axis=3, keepdims=True)).astype(jnp.bfloat16)
    attended = jnp.einsum(
        "rhqk,rkhd->rqhd", probs, value4, preferred_element_type=jnp.float32
    )
    attended = attended.astype(jnp.bfloat16).reshape(rows_here, head_cols)
    late = (early, output_weight.shape[0] - early, early)
    mixed, out_weights, _ = gather(
        (("split", "tp", 1), ("line", "rep", late), ("fill", "rep", 1)),
        sizes,
        (attended, output_weight, out_early),
        2,
    )
    out_weights = out_weights.reshape(-1, tokens.shape[1])
    update = jnp.dot(mixed, out_weights, preferred_element_type=jnp.float32)
    resid_out = (xfloat + update).astype(jnp.bfloat16)
    rfloat = resid_out.astype(jnp.float32)
    squares = jnp.sum(rfloat * rfloat, axis=1)
    local_scores = jnp.dot(rfloat * final_gain, value_head, precision=lax.Precision.HIGHEST)
    stats = jnp.concatenate([local_scores.T, squares[None, :]], axis=0)
    (stats_all,) = gather((("direct", "tp", None),), sizes, (stats,), 3)
    stats = jnp.sum(stats_all, axis=0)
    logits = (stats[:-1] * lax.rsqrt(stats[-1:] / width + EPS)).T
    live = (position[None, :] < row_lengths[:, None]).reshape(rows_here, 1)
    objective_scores = jnp.where(live, logits, jnp.float32(0.0))
    return (resid_out, objective_scores)


def solution(mesh):
    in_specs = (
        P("rep", "tp"),
        P("rep"),
        P("tp"),
        P("rep", "tp"),
        P("rep", "tp"),
        P("rep", "tp"),
        P("rep", "tp"),
        P("tp"),
        P("tp", None),
    )
    out_specs = (P("rep", "tp"), P("rep", None))
    body = functools.partial(local, dict(mesh.shape))
    return jax.shard_map(body, mesh=mesh, in_specs=in_specs, out_specs=out_specs, check_vma=False)
```

```python
import functools
import jax
import jax.numpy as jnp
from jax import lax
from jax.experimental import pallas as pl
from jax.experimental.pallas import tpu as pltpu
from jax.sharding import PartitionSpec as P

KEY_VALUE_HEADS = 4
HEAD_SIZE = 128
EPS = 1e-05
MESH = pl.DeviceIdType.MESH


class Stage:
    def __init__(self, src, dst, buffer, sems):
        self.into = pltpu.make_async_copy(src, buffer, sems.at[0])
        self.out = pltpu.make_async_copy(buffer, dst, sems.at[1])


def slot(ref, dim, size, index, rows=None):
    if rows is not None:
        return ref.at[pl.ds(*rows), pl.ds(pl.multiple_of(index * size, size), size)]
    if dim is None:
        return ref.at[index]
    if isinstance(dim, tuple):
        return ref.at[index, pl.ds(dim[2], dim[1])]
    start = pl.multiple_of(index * size, size)
    return ref.at[pl.ds(start, size)] if dim == 0 else ref.at[:, pl.ds(start, size)]


class Line:
    def __init__(self, axis, count, dim, src, dst, sems, rows=None):
        self.axis, self.dim, self.dst = axis, dim, dst
        self.windowed = isinstance(dim, tuple)
        rows = dim[:2] if self.windowed else rows
        self.src = src if rows is None else src.at[pl.ds(*rows)]
        self.rows = None if self.windowed else rows
        self.count = count
        self.up_sem, self.down_sem, self.pair_sem, self.line_recv, self.pair_recv = sems
        me = lax.axis_index(axis)
        self.me, self.place, self.side = me, me // 2, me % 2
        self.partner = me + 1 - 2 * self.side
        self.size = None if dim is None or self.windowed else src.shape[dim]

    def at(self, index):
        return slot(self.dst, self.dim, self.size, index, self.rows)

    def copy(self, source, index, send, recv, target):
        return pltpu.make_async_remote_copy(
            src_ref=source,
            dst_ref=self.at(index),
            send_sem=send,
            recv_sem=recv,
            device_id={self.axis: target},
            device_id_type=MESH,
        )

    def up(self, source, origin):
        return self.copy(
            source, 2 * origin + self.side, self.up_sem.at[origin], self.line_recv.at[origin], self.me + 2
        )

    def down(self, source, origin):
        return self.copy(
            source, 2 * origin + self.side, self.down_sem.at[origin], self.line_recv.at[origin], self.me - 2
        )

    def pair(self, source, origin):
        return self.copy(
            source,
            2 * origin + self.side,
            self.pair_sem.at[origin],
            self.pair_recv.at[origin],
            self.partner,
        )

    def own_block(self):
        return self.at(self.me)

    def has_up(self):
        return self.place < self.count - 1

    def has_down(self):
        return self.place > 0

    def begin(self):
        @pl.when(self.has_up())
        def _():
            self.up(self.src, self.place).start()

        @pl.when(self.has_down())
        def _():
            self.down(self.src, self.place).start()

        self.pair(self.src, self.place).start()

    def hop(self, step):
        below, above = self.place - step, self.place + step

        @pl.when(below >= 0)
        def _():
            block = self.at(2 * below + self.side)
            self.up(block, below).wait_recv()

            @pl.when(self.has_up())
            def _():
                self.up(block, below).start()

            self.pair(block, below).start()

        @pl.when(above < self.count)
        def _():
            block = self.at(2 * above + self.side)
            self.down(block, above).wait_recv()

            @pl.when(self.has_down())
            def _():
                self.down(block, above).start()

            self.pair(block, above).start()

    def finish(self):
        for origin in range(self.count):
            here = self.at(2 * origin + self.side)
            self.pair(here, origin).wait_send()
            pltpu.make_async_remote_copy(
                src_ref=here,
                dst_ref=self.at(2 * origin + 1 - self.side),
                send_sem=self.pair_sem.at[origin],
                recv_sem=self.pair_recv.at[origin],
                device_id={self.axis: self.partner},
                device_id_type=MESH,
            ).wait_recv()

            @pl.when((origin <= self.place) & self.has_up())
            def _():
                self.up(here, origin).wait_send()

            @pl.when((origin >= self.place) & self.has_down())
            def _():
                self.down(here, origin).wait_send()

    def neighbours(self):
        return ((self.has_up(), self.me + 2), (self.has_down(), self.me - 2), (None, self.partner))


class Cross(Line):
    def __init__(self, axis, count, dim, src, dst, sems, rows):
        super().__init__(axis, count, dim, src, dst, sems, rows)
        self.other = 1 - self.side

    def along(self, source, origin, side, which, step):
        sem = self.up_sem if step > 0 else self.down_sem
        return self.copy(
            source,
            2 * origin + side,
            sem.at[which * self.count + origin],
            self.line_recv.at[which * self.count + origin],
            self.me + step,
        )

    def spread(self, source, origin, which):
        side = self.side if which == 0 else self.other

        @pl.when(self.has_up() & (origin <= self.place))
        def _():
            self.along(source, origin, side, which, 2).start()

        @pl.when(self.has_down() & (origin >= self.place))
        def _():
            self.along(source, origin, side, which, -2).start()

    def across(self, index, source):
        return self.copy(source, index, self.pair_sem.at[0], self.pair_recv.at[0], self.partner)

    def begin(self):
        self.across(self.me, self.src).start()
        self.spread(self.src, self.place, 0)

    def turn(self):
        theirs = self.at(self.partner)
        self.across(self.partner, theirs).wait_recv()
        self.spread(theirs, self.place, 1)

    def hop(self, step):
        for which in range(2):
            side = self.side if which == 0 else self.other
            for origin in (self.place - step, self.place + step):

                @pl.when((origin >= 0) & (origin < self.count))
                def _(origin=origin, side=side, which=which):
                    block = self.at(2 * origin + side)
                    self.along(block, origin, side, which, 2).wait_recv()
                    self.spread(block, origin, which)

    def finish(self):
        self.across(self.me, self.src).wait_send()
        for which in range(2):
            side = self.side if which == 0 else self.other
            for origin in range(self.count):
                block = self.at(2 * origin + side)

                @pl.when((origin <= self.place) & self.has_up())
                def _(origin=origin, side=side, which=which, block=block):
                    self.along(block, origin, side, which, 2).wait_send()

                @pl.when((origin >= self.place) & self.has_down())
                def _(origin=origin, side=side, which=which, block=block):
                    self.along(block, origin, side, which, -2).wait_send()


class Direct:
    def __init__(self, axis, members, src, dst, sems):
        self.axis, self.members, self.src, self.dst = axis, members, src, dst
        self.send, self.recv = sems
        self.me = lax.axis_index(axis)

    def to(self, offset):
        return pltpu.make_async_remote_copy(
            src_ref=self.src,
            dst_ref=self.dst.at[self.me],
            send_sem=self.send.at[offset - 1],
            recv_sem=self.recv.at[offset - 1],
            device_id={self.axis: lax.rem(self.me + offset, self.members)},
            device_id_type=MESH,
        )

    def come(self, offset):
        return pltpu.make_async_remote_copy(
            src_ref=self.src,
            dst_ref=self.dst.at[lax.rem(self.me - offset + self.members, self.members)],
            send_sem=self.send.at[offset - 1],
            recv_sem=self.recv.at[offset - 1],
            device_id={self.axis: lax.rem(self.me + offset, self.members)},
            device_id_type=MESH,
        )

    def own_block(self):
        return self.dst.at[self.me]

    def begin(self):
        for offset in range(1, self.members):
            self.to(offset).start()

    def finish(self):
        for offset in range(1, self.members):
            self.to(offset).wait_send()
            self.come(offset).wait_recv()


def gather_kernel(plan, sizes, *refs):
    count = len(plan)
    sources, targets = refs[:count], refs[count : 2 * count]
    rest = list(refs[2 * count :])

    def take(number):
        taken = rest[:number]
        del rest[:number]
        return taken

    jobs, stages = [], []
    for (kind, axis, dim), src, dst in zip(plan, sources, targets):
        if kind == "fill":
            dst = targets[dim]
            buffer, sems = take(2)
            stages.append(Stage(src, dst.at[:, pl.ds(axis, src.shape[1])], buffer, sems))
            continue
        if kind == "direct":
            made = [Direct(axis, sizes[axis], src, dst, take(2))]
        elif kind == "line":
            made = [Line(axis, sizes[axis] // 2, dim, src, dst, take(5))]
        else:
            first, second = cut(src.shape[0])
            made = [
                Line(axis, sizes[axis] // 2, dim, src, dst, take(5), first),
                Cross(axis, sizes[axis] // 2, dim, src, dst, take(5), second),
            ]
        for job in made:
            buffer, sems = take(2)
            stages.append(Stage(job.src, job.own_block(), buffer, sems))
        jobs += made
    barrier = pltpu.get_barrier_semaphore()
    direct_axes = {job.axis for job in jobs if isinstance(job, Direct)}
    greeted, peers = set(), 0
    for job in jobs:
        if job.axis in greeted:
            continue
        greeted.add(job.axis)
        if job.axis in direct_axes:
            members = sizes[job.axis]
            peers = peers + members - 1
            for offset in range(1, members):
                pl.semaphore_signal(
                    barrier,
                    inc=1,
                    device_id={job.axis: lax.rem(job.me + offset, members)},
                    device_id_type=MESH,
                )
        else:
            for there, target in job.neighbours():
                def signal(target=target, job=job):
                    pl.semaphore_signal(
                        barrier, inc=1, device_id={job.axis: target}, device_id_type=MESH
                    )

                if there is None:
                    peers = peers + 1
                    signal()
                else:
                    peers = peers + there.astype(jnp.int32)
                    pl.when(there)(signal)
    pl.semaphore_wait(barrier, peers)
    for job in jobs:
        job.begin()
    for stage in stages:
        stage.into.start()
    for stage in stages:
        stage.into.wait()
        stage.out.start()
    for job in jobs:
        if isinstance(job, Cross):
            job.turn()
    for axis in ("tp", "rep"):
        lines = [job for job in jobs if isinstance(job, Line) and job.axis == axis]
        for step in range(1, max([job.count for job in lines], default=1)):
            for job in lines:
                job.hop(step)
    for job in jobs:
        job.finish()
    for stage in stages:
        stage.out.wait()


def cut(total):
    cross = total // (6 * 16) * 16
    return (0, total - cross), (total - cross, cross)


def gather(plan, sizes, arrays, collective_id, memory=pl.ANY):
    shapes, scratch = [], []
    dma = pltpu.SemaphoreType.DMA
    for (kind, axis, dim), array in zip(plan, arrays):
        if kind == "fill":
            shapes.append(jax.ShapeDtypeStruct((8, 128), array.dtype))
            scratch += [pltpu.VMEM(array.shape, array.dtype), dma((2,))]
            continue
        members = sizes[axis]
        if dim is None:
            shape = (members,) + array.shape
        elif isinstance(dim, tuple):
            shape = (members, dim[2] + dim[1]) + array.shape[1:]
        else:
            shape = tuple(n * members if i == dim else n for i, n in enumerate(array.shape))
        shapes.append(jax.ShapeDtypeStruct(shape, array.dtype))
        whole = pltpu.VMEM(array.shape, array.dtype)
        if kind == "direct":
            scratch += [dma((members - 1,))] * 2 + [whole, dma((2,))]
        elif kind == "line":
            if isinstance(dim, tuple):
                whole = pltpu.VMEM(dim[1:2] + array.shape[1:], array.dtype)
            scratch += [dma((members // 2,))] * 5 + [whole, dma((2,))]
        else:
            scratch += [dma((members // 2,))] * 5 + [dma((members,))] * 5
            for _, length in cut(array.shape[0]):
                scratch += [pltpu.VMEM((length,) + array.shape[1:], array.dtype), dma((2,))]
    return pl.pallas_call(
        functools.partial(gather_kernel, plan, sizes),
        out_shape=tuple(shapes),
        in_specs=[pl.BlockSpec(memory_space=memory)] * len(arrays),
        out_specs=tuple([pl.BlockSpec(memory_space=memory)] * len(arrays)),
        scratch_shapes=scratch,
        compiler_params=pltpu.CompilerParams(collective_id=collective_id, has_side_effects=True),
    )(*arrays)


def local(
    sizes,
    tokens,
    row_lengths,
    attn_gain,
    query_weight,
    key_weight,
    value_matrix,
    output_weight,
    final_gain,
    value_head,
):
    width = tokens.shape[1] * sizes["tp"]
    rows_here = tokens.shape[0]
    head_cols = query_weight.shape[1]
    kv_cols = key_weight.shape[1]
    xfloat = tokens.astype(jnp.float32)
    squares_here = jnp.sum(xfloat * xfloat, axis=1)[None, :]
    gained = (xfloat * attn_gain).astype(jnp.bfloat16)
    packed = jnp.concatenate([query_weight, key_weight, value_matrix], axis=1)
    first = output_weight.shape[0] // 16
    early = output_weight.shape[0] // 4
    columns, weights, out_first, squares_all = gather(
        (
            ("split", "tp", 1),
            ("line", "rep", 0),
            ("line", "rep", (0, first, 0)),
            ("direct", "tp", None),
        ),
        sizes,
        (gained, packed, output_weight, squares_here),
        0,
    )
    first_scale = lax.rsqrt(jnp.sum(squares_all, axis=(0, 1)) / width + EPS)[:, None]
    projected = jnp.dot(columns, weights, preferred_element_type=jnp.float32)
    projected = (projected * first_scale).astype(jnp.bfloat16)
    query = projected[:, :head_cols]
    kv_all, out_early = gather(
        (("line", "tp", None), ("line", "rep", (first, early, 0))),
        sizes,
        (projected[:, head_cols:], output_weight),
        1,
    )
    sequence_rows = row_lengths.shape[0]
    length = rows_here // sequence_rows
    local_heads = head_cols // HEAD_SIZE
    key_full = kv_all[:, :, :kv_cols].transpose(1, 0, 2).reshape(rows_here, -1)
    value_full = kv_all[:, :, kv_cols:].transpose(1, 0, 2).reshape(rows_here, -1)
    first_head = lax.axis_index("tp") * local_heads
    key_value_index = (first_head + jnp.arange(local_heads, dtype=jnp.int32)) % KEY_VALUE_HEADS
    query4 = query.reshape(sequence_rows, length, local_heads, HEAD_SIZE)
    key4 = key_full.reshape(sequence_rows, length, KEY_VALUE_HEADS, HEAD_SIZE)
    value4 = value_full.reshape(sequence_rows, length, KEY_VALUE_HEADS, HEAD_SIZE)
    if local_heads % KEY_VALUE_HEADS or local_heads != KEY_VALUE_HEADS:
        key4 = jnp.take(key4, key_value_index, axis=2)
        value4 = jnp.take(value4, key_value_index, axis=2)
    scores = jnp.einsum(
        "rqhd,rkhd->rhqk", query4, key4, preferred_element_type=jnp.float32
    ) * (1.0 / HEAD_SIZE**0.5)
    position = jnp.arange(length, dtype=jnp.int32)
    causal = position[None, :] <= position[:, None]
    allowed = causal[None, None, :, :] & (
        position[None, None, None, :] < row_lengths[:, None, None, None]
    )
    scores = jnp.where(allowed, scores, jnp.float32(-1e30))
    scores = scores - jnp.max(scores, axis=3, keepdims=True)
    expo = jnp.exp(scores)
    probs = (expo / jnp.sum(expo, axis=3, keepdims=True)).astype(jnp.bfloat16)
    attended = jnp.einsum(
        "rhqk,rkhd->rqhd", probs, value4, preferred_element_type=jnp.float32
    )
    attended = attended.astype(jnp.bfloat16).reshape(rows_here, head_cols)
    before = first + early
    late = (before, output_weight.shape[0] - before, before)
    mixed, out_weights, _, _ = gather(
        (("split", "tp", 1), ("line", "rep", late), ("fill", 0, 1), ("fill", first, 1)),
        sizes,
        (attended, output_weight, out_first, out_early),
        2,
    )
    out_weights = out_weights.reshape(-1, tokens.shape[1])
    update = jnp.dot(mixed, out_weights, preferred_element_type=jnp.float32)
    resid_out = (xfloat + update).astype(jnp.bfloat16)
    rfloat = resid_out.astype(jnp.float32)
    squares = jnp.sum(rfloat * rfloat, axis=1)
    local_scores = jnp.dot(rfloat * final_gain, value_head, precision=lax.Precision.HIGHEST)
    stats = jnp.concatenate([local_scores.T, squares[None, :]], axis=0)
    (stats_all,) = gather((("direct", "tp", None),), sizes, (stats,), 3)
    stats = jnp.sum(stats_all, axis=0)
    logits = (stats[:-1] * lax.rsqrt(stats[-1:] / width + EPS)).T
    live = (position[None, :] < row_lengths[:, None]).reshape(rows_here, 1)
    objective_scores = jnp.where(live, logits, jnp.float32(0.0))
    return (resid_out, objective_scores)


def solution(mesh):
    in_specs = (
        P("rep", "tp"),
        P("rep"),
        P("tp"),
        P("rep", "tp"),
        P("rep", "tp"),
        P("rep", "tp"),
        P("rep", "tp"),
        P("tp"),
        P("tp", None),
    )
    out_specs = (P("rep", "tp"), P("rep", None))
    body = functools.partial(local, dict(mesh.shape))
    return jax.shard_map(body, mesh=mesh, in_specs=in_specs, out_specs=out_specs, check_vma=False)
```
